32 devices in a mesh: groups: 2 (over x), ep: 8 (over z, y), rep: 2 (over core).
Axes of the slice: x: 2, y: 2, z: 4, core: 2. Of those that a mesh axis runs over, the one named last changes fastest.
Arguments:
- tokens: bfloat16 [512, 3584], P(('groups', 'ep'), 'rep'), parts along dimension 0, may hold values from -6 to 6
- expert_ids: int32 [512, 1], P(('groups', 'ep')), parts along dimension 0, may hold values from 0 to 3; in each aligned block of 32 rows (0 to 31, 32 to 63, ...) at most 10 rows name the same one
- gate_values: float32 [512, 1], P(('groups', 'ep')), parts along dimension 0, may hold values from 0.1 to 0.6
- slot_expert: int32 [8], replicated, may hold values from 0 to 3, as said below
- gate_weight: bfloat16 [8, 3584, 1024], P('ep', None, 'rep'), as said below
- up_weight: bfloat16 [8, 3584, 1024], P('ep', None, 'rep'), as said below
- down_weight: bfloat16 [8, 1024, 3584], P('ep', 'rep'), as said below
Outputs:
- combined: bfloat16 [512, 3584], P(('groups', 'ep'), 'rep'), parts along dimension 0
The draws below stay inside these ranges and needn't reach their ends.
There are 2 independent parts, one for each index of `groups`. The reference program is written for one: setup_inputs(seed, part) draws one part's arguments, and reference() takes and returns one part's arrays. A program takes and returns all parts, laid end to end along the dimension named above; an argument that names none is the same for every part. Nothing has to cross between parts.
Inputs may be any that keep to these rules, and one draw needn't show every extreme that they name: `expert_ids`: each row names 1 different experts. Among the 32 rows of one index of ep (aligned blocks) no expert is named more than 10 times, and in some blocks one expert is named exactly 10 times. `slot_expert`: every expert is held by 1 to 4 slots, and some experts by 4. gate_weight[s] equals gate_weight[r] whenever slot_expert[s] equals slot_expert[r]. up_weight[s] equals up_weight[r] whenever slot_expert[s] equals slot_expert[r]. down_weight[s] equals down_weight[r] whenever slot_expert[s] equals slot_expert[r].
All inputs are finite; a program needn't handle non-finite values.
Results may differ from the reference program's by a relative error of at most 0.0057.
Values may be sent and summed in bfloat16 or wider, within the bound.
A program may use at most 128 MiB of HBM per device.

```python
import math
import jax
import jax.numpy as jnp
import numpy as np
from jax import lax

D = 3584
HID = 1024
TOK_EP = 32
EXPERTS = 4
TOP = 1
CAP = 10
TOKENS = 256
N_EP = 8


def plan_of(key):
    plan_key = jax.random.fold_in(key, 11)
    first_key, second_key = jax.random.split(plan_key)
    ordering = jax.random.permutation(first_key, EXPERTS)
    ranked = jnp.arange(EXPERTS)
    quarter = EXPERTS // 4
    copies = jnp.where(ranked < quarter, 4, jnp.where(ranked < 2 * quarter, 2, 1))
    listing = jnp.repeat(ordering, copies, total_repeat_length=2 * EXPERTS)
    shuffle = jax.random.permutation(second_key, 2 * EXPERTS)
    return listing[shuffle].astype(jnp.int32)


def slot_weights(key, salt_value, row_count, col_count):
    holders = plan_of(key)
    weight_key = jax.random.fold_in(key, salt_value)
    spread = 1.0 / math.sqrt(row_count)

    def one_slot(expert):
        return jax.random.normal(jax.random.fold_in(weight_key, expert), (row_count, col_count), jnp.float32) * spread
    return jax.vmap(one_slot)(holders)


def draw_slot_expert(key, part):
    return plan_of(key)


def draw_gate_weight(key, part):
    return slot_weights(key, 21, D, HID).astype(jnp.bfloat16)


def draw_up_weight(key, part):
    return slot_weights(key, 22, D, HID).astype(jnp.bfloat16)


def draw_down_weight(key, part):
    return slot_weights(key, 23, HID, D).astype(jnp.bfloat16)


def steps_of(rng, extent, cuts, least, largest):
    gain, own = 1.0, jax.random.fold_in(rng, 6)
    for dim, blocks in cuts:
        heights = jnp.exp(jax.random.uniform(jax.random.fold_in(own, dim), (blocks,), jnp.float32, least / len(cuts), largest / len(cuts)))
        gain = gain * jnp.repeat(heights, extent[dim] // blocks).reshape([-1 if axis == dim else 1 for axis in range(len(extent))])
    return gain


def assign_block(own_key, own, number, rows, number_of, top, limit, skew):
    sequence = jax.random.permutation(own_key, number_of)
    packed, usual = load_shares(number_of, rows * top, limit, skew, True), load_shares(number_of, rows * top, limit, skew, False)
    places = jnp.arange(number_of)

    def named(tallies, rotation):
        used = int((tallies > 0).sum())
        fixed = max(1, used // 4)
        passed = fixed + (places - fixed + rotation * (used - fixed)) % max(1, number_of - fixed)
        return jnp.zeros((number_of,), jnp.int32).at[sequence[jnp.where(places < fixed, places, passed)]].set(jnp.asarray(tallies, jnp.int32))

    tallies = jnp.where(number % 4 == 0, named(packed, number // 4), named(usual, number - number // 4 - 1))
    mixed = jax.random.permutation(jax.random.fold_in(own, 3), number_of)
    giver, receiver = mixed[0:number_of // 2 * 2:2], mixed[1:number_of // 2 * 2:2]
    margin = jnp.minimum(tallies[giver] - 1, limit - tallies[receiver]) // 2
    margin = jnp.where((giver == sequence[0]) | (receiver == sequence[0]) | (tallies[receiver] == 0), 0, jnp.maximum(margin, 0))
    passed = jax.random.randint(jax.random.fold_in(own, 4), (number_of // 2,), 0, 1 << 20) % (margin + 1)
    tallies = tallies.at[giver].add(-passed).at[receiver].add(passed)
    items = jnp.searchsorted(jnp.cumsum(tallies), jnp.arange(rows * top), side="right").astype(jnp.int32)
    table = items.reshape(top, rows).T
    table = table[jax.random.permutation(jax.random.fold_in(own, 1), rows)]
    rotation = jax.random.randint(jax.random.fold_in(own, 2), (rows, 1), 0, top)
    return jnp.take_along_axis(table, (jnp.arange(top)[None, :] + rotation) % top, axis=1)


def load_shares(number_of, total, reach, skew, full):
    loads = [(1 << 20) // math.isqrt(grade ** skew) + 1 for grade in range(1, number_of + 1)]
    largest = reach if full else min(reach, max(-(-total // number_of), total * loads[0] // sum(loads)))
    least = 1 if total - largest >= number_of - 1 else 0
    counts, rest = [largest] + [least] * (number_of - 1), total - largest - least * (number_of - 1)
    while rest > 0:
        movable = [i for i in range(1, number_of) if counts[i] < largest] or [i for i in range(1, number_of) if counts[i] < reach]
        mass, budget = sum([loads[i] for i in movable]), rest
        for i in movable:
            addition = min(reach - counts[i], max(1, budget * loads[i] // mass), rest)
            counts[i] = counts[i] + addition
            rest = rest - addition
    return np.array(counts)


def scatter_about(key, dims, deviation, reach, pieces=(), held_as=jnp.bfloat16):
    drawn = jax.random.normal(key, dims, jnp.float32) * deviation
    if len(pieces) > 0:
        drawn = steps_of(key, dims, pieces, -0.22, 0.18) * drawn
    return jnp.clip(drawn, min=-reach, max=reach).astype(held_as)


def setup_inputs(seed: int = 0, part: int = 0) -> dict:
    seeds = jax.random.split(jax.random.key(seed), 8)
    own_keys = jax.random.split(jax.random.fold_in(seeds[7], part), 8)
    tokens = scatter_about(own_keys[0], (TOKENS, D), 1.0, 6.0, ((0, 8), (1, 2)))
    expert_ids_keys = jax.random.split(jax.random.fold_in(own_keys[1], 1), TOKENS // TOK_EP)
    expert_ids_turns = jax.random.permutation(jax.random.fold_in(own_keys[1], 3), TOKENS // TOK_EP)
    expert_ids = jax.vmap(lambda own, number: assign_block(jax.random.fold_in(own_keys[1], 2), own, number, TOK_EP, EXPERTS, TOP, CAP, 2))(expert_ids_keys, expert_ids_turns).reshape((TOKENS, TOP))
    gate_values = jnp.clip(0.1 + 0.5 * jax.random.uniform(own_keys[2], (TOKENS, TOP), jnp.float32) ** steps_of(own_keys[2], (TOKENS, TOP), ((0, 8),), -0.2, 0.2), 0.1, 0.6)
    slot_expert = draw_slot_expert(jax.random.fold_in(seeds[7], 71), part)
    gate_weight = draw_gate_weight(jax.random.fold_in(seeds[7], 71), part)
    up_weight = draw_up_weight(jax.random.fold_in(seeds[7], 71), part)
    down_weight = draw_down_weight(jax.random.fold_in(seeds[7], 71), part)
    return {"tokens": tokens, "expert_ids": expert_ids, "gate_values": gate_values, "slot_expert": slot_expert, "gate_weight": gate_weight, "up_weight": up_weight, "down_weight": down_weight}


def reference(tokens, expert_ids, gate_values, slot_expert, gate_weight, up_weight, down_weight):
    pair_count = TOKENS * TOP
    row_bound = min(pair_count, N_EP * CAP)
    pair_expert = expert_ids.reshape(pair_count)
    padded = jnp.concatenate([tokens, jnp.zeros((1, D), tokens.dtype)], axis=0)
    flat_gates = jnp.concatenate([gate_values.reshape(pair_count), jnp.zeros((1,), gate_values.dtype)], axis=0)

    def one_expert(running, expert):
        slot_index = jnp.argmax(slot_expert == expert).astype(jnp.int32)
        members = jnp.nonzero(pair_expert == expert, size=row_bound, fill_value=pair_count)[0].astype(jnp.int32)
        row_block = padded[members // TOP]
        gate_proj = jnp.dot(row_block, gate_weight[slot_index], preferred_element_type=jnp.float32)
        up_proj = jnp.dot(row_block, up_weight[slot_index], preferred_element_type=jnp.float32)
        hidden = (jax.nn.silu(gate_proj) * up_proj).astype(jnp.bfloat16)
        outcome = jnp.dot(hidden, down_weight[slot_index], preferred_element_type=jnp.float32).astype(jnp.bfloat16)
        weight = flat_gates[members]
        running = running.at[members // TOP].add(weight[:, None] * outcome.astype(jnp.float32))
        return running, None

    running, _ = lax.scan(one_expert, jnp.zeros((TOKENS + 1, D), jnp.float32), jnp.arange(EXPERTS, dtype=jnp.int32))
    return running[:TOKENS].astype(jnp.bfloat16)
```

```python
import functools

import jax
import jax.numpy as jnp
from jax import lax
from jax.experimental import pallas as pl
from jax.experimental.pallas import tpu as pltpu
from jax.sharding import PartitionSpec as P

MESH = pl.DeviceIdType.MESH
F32 = jnp.float32
BF16 = jnp.bfloat16
HEAD = 8


def iota(shape, dim):
    return lax.broadcasted_iota(jnp.int32, shape, dim)


def repeat(low, high, step):
    if high - low <= 8:
        for i in reversed(range(low, high)):
            step(i)
    else:
        lax.fori_loop(0, high - low, lambda i, c: (step(high - 1 - i), c)[1], 0)


def mix(n, a, b):
    total, bit = 0, 1
    while bit < n:
        total = total + (a // bit + b // bit) % 2 * bit
        bit *= 2
    return total


def routing(ids, slots_row, ep, tail):
    top, rows = ids.shape
    n = slots_row.shape[1]
    at_row, at_col = iota((n, n), 0), iota((n, n), 1)
    slots_all = jnp.broadcast_to(slots_row, (n, n))
    slots_col = jnp.sum(jnp.where(at_row == at_col, slots_all, 0), axis=1, keepdims=True)
    same = slots_col == slots_all
    copies = jnp.sum(jnp.where(same, 1, 0), axis=1, keepdims=True)
    rank = jnp.sum(jnp.where(same & (at_col < at_row), 1, 0), axis=1, keepdims=True)
    want = jnp.zeros_like(copies)
    for c in range(2, 5):
        want = jnp.where(copies == c, lax.rem(ep, c), want)
    goes = jnp.zeros((n, rows), F32)
    for k in range(top):
        hit = (ids[k : k + 1, :] == slots_col) & (rank == want)
        goes = jnp.where(hit, 1.0, goes)
    before = jnp.where(iota((rows, rows), 0) < iota((rows, rows), 1), 1.0, 0.0)
    place = jnp.dot(goes, before, preferred_element_type=F32)
    r, s = iota((n * HEAD, n), 0), iota((n * HEAD, n), 1)
    m = place_of(n, ep, jnp.bitwise_xor(s, ep))
    mine = (r >= m * HEAD) & (r < m * HEAD + HEAD)
    spread = jnp.where(mine, 1.0, 0.0)
    index = jnp.sum(jnp.where(mine, r - m * HEAD, 0), axis=1, keepdims=True)
    experts = jnp.sum(
        jnp.where(mine, jnp.broadcast_to(slots_row, (n * HEAD, n)), 0), axis=1, keepdims=True
    )
    goes_r = jnp.dot(spread, goes, preferred_element_type=F32)
    place_r = jnp.dot(spread, place, preferred_element_type=F32)
    place_in = jnp.where(goes_r > 0.5, place_r, -1.0)
    heads = jnp.where(place_in == index.astype(F32), 1.0, 0.0)
    folds = []
    for q in range(HEAD // tail):
        wanted = jnp.where((index >= q * tail) & (index < q * tail + tail), index - q * tail + HEAD, -2)
        folds.append(jnp.where(place_in == wanted.astype(F32), 1.0, 0.0))
    return heads, folds, experts


def fold_width(half, tail):
    return (half * tail // HEAD + 127) // 128 * 128


def fold_cuts(half, tail):
    wide = fold_width(half, tail)
    return [(q * wide, min(wide, half - q * wide)) for q in range(HEAD // tail)]


def widen(piece, wide):
    short = wide - piece.shape[1]
    return jnp.concatenate([piece, jnp.zeros((piece.shape[0], short), piece.dtype)], 1) if short else piece


def place_of(n, ep, mask):
    width = grid_width(n)
    if n // width != 4:
        return mask
    row = ep // width
    inner = (row // 2 + row) % 2
    far = jnp.where(mask >= 2 * width, 1, 0)
    last = jnp.where(mask >= 3 * width, 1, 0)
    return mask + far * inner * (1 - 2 * last) * width


def kernel(n, cap, tok_hbm, ids_hbm, slots_hbm, gates_hbm, wg_hbm, wu_hbm, wd_hbm, out_ref,
           tok, ids_ref, slots_ref, gates_ref, in_sem,
           wg, wu, wd, w_sem, d_send, d_recv, s_send, s_recv, f_send, f_recv, h_send, h_recv,
           r_send, r_recv, ready, send, x, res, ret, *waves):
    ep, rep = lax.axis_index("ep"), lax.axis_index("rep")
    other = 1 - rep
    rows, half = tok.shape
    tail = cap - HEAD
    cuts, wide = fold_cuts(half, tail), fold_width(half, tail)

    barrier = pltpu.get_barrier_semaphore()

    width = grid_width(n)
    height = n // width
    row, col = ep // width, ep % width
    beside = (
        (row > 0, ep - width), (row < height - 1, ep + width), (col > 0, ep - 1), (col < width - 1, ep + 1),
    )
    near_count = sum(jnp.where(there, 1, 0) for there, _ in beside)

    def tell(sem):
        for there, peer in beside:

            @pl.when(there)
            def _():
                pl.semaphore_signal(sem, inc=1, device_id={"ep": peer}, device_id_type=MESH)

    tell(barrier)
    pl.semaphore_signal(barrier, inc=1, device_id={"rep": other}, device_id_type=MESH)

    inputs = [
        pltpu.make_async_copy(ids_hbm, ids_ref, in_sem.at[0]),
        pltpu.make_async_copy(slots_hbm, slots_ref, in_sem.at[1]),
        pltpu.make_async_copy(tok_hbm, tok, in_sem.at[2]),
        pltpu.make_async_copy(gates_hbm, gates_ref, in_sem.at[3]),
    ]
    for copy in inputs:
        copy.start()
    def greet():
        pl.semaphore_wait(barrier, near_count + 1)
        if height + width > 3:
            tell(ready.at[0])

    pl.when(row == height - 1)(greet)
    inputs[0].wait()
    inputs[1].wait()
    inputs[2].wait()
    weights = [
        pltpu.make_async_copy(wg_hbm.at[0], wg, w_sem.at[0]),
        pltpu.make_async_copy(wu_hbm.at[0], wu, w_sem.at[1]),
        pltpu.make_async_copy(
            wd_hbm.at[0, :, pl.ds(pl.multiple_of(rep * half, 128), half)], wd.at[rep], w_sem.at[2]
        ),
    ]
    for copy in weights:
        copy.start()

    heads, folds, experts = routing(ids_ref[...], slots_ref[...], ep, tail)
    tokens = tok[...]

    def shape_up(block):
        return block.astype(BF16).reshape(block.shape[0] // HEAD, HEAD, block.shape[1])

    send[:, :, :half] = shape_up(jnp.dot(heads.astype(BF16), tokens, preferred_element_type=F32))
    folded = None
    for (at, size), pick in zip(cuts, folds):
        piece = jnp.dot(pick.astype(BF16), tokens[:, at : at + size], preferred_element_type=F32)
        piece = widen(piece, wide)
        folded = piece if folded is None else folded + piece
    send[:, :, half:] = shape_up(folded)
    inputs[3].wait()

    pl.when(row < height - 1)(greet)

    def down(side):
        return pltpu.make_async_remote_copy(
            src_ref=wd_hbm.at[0, :, pl.ds(pl.multiple_of(other * half, 128), half)],
            dst_ref=wd.at[side], send_sem=d_send, recv_sem=d_recv,
            device_id={"rep": other}, device_id_type=MESH,
        )

    def peer_of(p):
        mask = place_of(n, ep, p)
        peer = mix(n, ep, mask)
        return peer, place_of(n, peer, mask)

    def packet(p):
        peer, there = peer_of(p)
        return pltpu.make_async_remote_copy(
            src_ref=send.at[p], dst_ref=x.at[rep, there],
            send_sem=s_send.at[p], recv_sem=s_recv.at[there],
            device_id={"ep": peer}, device_id_type=MESH,
        )

    def arrival(p):
        peer, _ = peer_of(p)
        return pltpu.make_async_remote_copy(
            src_ref=send.at[p], dst_ref=x.at[rep, p],
            send_sem=s_send.at[p], recv_sem=s_recv.at[p],
            device_id={"ep": peer}, device_id_type=MESH,
        )

    def forward(p, side):
        return pltpu.make_async_remote_copy(
            src_ref=x.at[side, p], dst_ref=x.at[side, p],
            send_sem=f_send.at[p], recv_sem=f_recv.at[p],
            device_id={"rep": other}, device_id_type=MESH,
        )

    def back(p):
        peer, there = peer_of(p)
        return pltpu.make_async_remote_copy(
            src_ref=res.at[p], dst_ref=ret.at[there],
            send_sem=r_send.at[p], recv_sem=r_recv.at[there],
            device_id={"ep": peer}, device_id_type=MESH,
        )

    def returned(p):
        peer, _ = peer_of(p)
        return pltpu.make_async_remote_copy(
            src_ref=res.at[p], dst_ref=ret.at[p],
            send_sem=r_send.at[p], recv_sem=r_recv.at[p],
            device_id={"ep": peer}, device_id_type=MESH,
        )

    def start_packet(p):
        packet(p).start()

    def distance(peer):
        there, place = peer // width, peer % width
        return jnp.where(there > row, there - row, row - there) + jnp.where(place > col, place - col, col - place)

    reach = height + width - 2
    for away in range(1, reach + 1):
        if away > 1:
            pl.semaphore_wait(ready.at[away - 2], near_count)
        if 1 < away < reach:
            tell(ready.at[away - 1])
        if n <= 8:
            for p in range(1, n):
                pl.when(distance(peer_of(p)[0]) == away)(functools.partial(start_packet, p))
    if n > 8:
        repeat(1, n, start_packet)
    down(rep).start()
    x[rep, 0] = send[0]
    forward(0, rep).start()

    def pass_on(p):
        arrival(p).wait_recv()
        forward(p, rep).start()

    def each(low, high, step):
        if high - low <= 8:
            for p in range(low, high):
                step(p)
        else:
            lax.fori_loop(low, high, lambda p, c: (step(p), c)[1], 0)

    over = (((0,), (0,)), ((), ()))

    def wave(w, low, high, hid, mid, gate_mid, up_mid):
        count = high - low

        def share(side):
            return pltpu.make_async_remote_copy(
                src_ref=hid.at[side], dst_ref=hid.at[side], send_sem=h_send.at[w], recv_sem=h_recv.at[w],
                device_id={"rep": other}, device_id_type=MESH,
            )

        def tails(block):
            rows_of = [
                block[:, q * tail : q * tail + tail, :size].reshape(count * tail, size)
                for q, (_, size) in enumerate(cuts)
            ]
            return jnp.concatenate(rows_of, axis=1)

        def add(gate, up, side):
            upper = x[side, low:high, :, :half].reshape(count * HEAD, half)
            block = jnp.concatenate([upper, tails(x[side, low:high, :, half:])], axis=0)
            lines = pl.ds(pl.multiple_of(side * half, 128), half)
            g = jnp.dot(block, wg[lines, :], preferred_element_type=F32)
            u = jnp.dot(block, wu[lines, :], preferred_element_type=F32)
            return (g, u) if gate is None else (gate + g, up + u)

        each(max(low, 1), high, pass_on)
        if w == 0:
            weights[0].wait()
            weights[1].wait()
        gate_mid[...], up_mid[...] = add(None, None, rep)
        each(low, high, lambda p: forward(p, other).wait_recv())
        gate, up = add(gate_mid[...], up_mid[...], other)
        hid[rep] = ((gate / (1.0 + jnp.exp(-gate))) * up).astype(BF16)
        share(rep).start()
        if w == 0:
            weights[2].wait()
        mid[...] = jnp.dot(hid[rep], wd[rep], preferred_element_type=F32)
        if w == 0:
            down(other).wait_recv()
        share(other).wait_recv()
        result = mid[...] + jnp.dot(hid[other], wd[other], preferred_element_type=F32)
        split = count * HEAD
        res[low:high, :, :half] = shape_up(result[:split])
        last = result[split:].astype(BF16)
        for q, (at, size) in enumerate(cuts):
            piece = widen(last[:, at : at + size], wide).reshape(count, tail, wide)
            res[low:high, q * tail : q * tail + tail, half:] = piece
        repeat(max(low, 1), high, lambda p: back(p).start())
        share(rep).wait_send()

    def run(cuts_at, buffers):
        for w, (low, high) in enumerate(zip((0,) + cuts_at, cuts_at + (n,))):
            wave(w, low, high, *buffers[4 * w : 4 * w + 4])

    plans = wave_plans(n)
    at = 0
    for kind, cuts_at in enumerate(plans):
        span = 4 * (len(cuts_at) + 1)
        step = functools.partial(run, cuts_at, waves[at : at + span])
        at += span
        if len(plans) == 1:
            step()
        else:
            pl.when((row // 2 + row) % 2 == kind)(step)
    ret[0] = res[0]

    down(rep).wait_send()

    def sent(p):
        packet(p).wait_send()
        forward(p, rep).wait_send()

    repeat(1, n, sent)
    forward(0, rep).wait_send()
    def got_back(p):
        returned(p).wait_recv()

    each(1, n, got_back)

    ids = ids_ref[...]
    gates = gates_ref[...]
    all_heads = ret[:, :, :half].reshape(n * HEAD, half)
    all_folds = ret[:, :, half:].reshape(n * HEAD, wide)
    diagonal = iota((rows, rows), 0) == iota((rows, rows), 1)
    total = None
    for k in range(ids.shape[0]):
        named = ids[k : k + 1, :] == experts
        hit = jnp.where(named, heads, 0.0).astype(BF16)
        got = lax.dot_general(hit, all_heads, over, preferred_element_type=F32)
        pieces = []
        for (_, size), pick in zip(cuts, folds):
            hit = jnp.where(named, pick, 0.0).astype(BF16)
            pieces.append(lax.dot_general(hit, all_folds[:, :size], over, preferred_element_type=F32))
        got = got + jnp.concatenate(pieces, axis=1)
        line = jnp.broadcast_to(gates[k : k + 1, :], (rows, rows))
        column = jnp.sum(jnp.where(diagonal, line, 0.0), axis=1, keepdims=True)
        total = got * column if total is None else total + got * column
    out_ref[...] = total

    repeat(1, n, lambda p: back(p).wait_send())


def grid_width(n):
    width = 1
    while width * width * 4 <= n:
        width *= 2
    return width


def wave_plans(n):
    return [()]


def body(tokens, expert_ids, gate_values, slot_expert, gate_weight, up_weight, down_weight):
    rows, top = expert_ids.shape
    half = tokens.shape[1]
    n = slot_expert.shape[0]
    experts = n // 2
    cap = rows * top * 5 // (4 * experts)
    tail = cap - HEAD
    depth, hidden = gate_weight.shape[1:]
    vmem = pl.BlockSpec(memory_space=pltpu.VMEM)
    hbm = pl.BlockSpec(memory_space=pl.ANY)
    dma = pltpu.SemaphoreType.DMA
    wide = half + fold_width(half, tail)

    combined = pl.pallas_call(
        functools.partial(kernel, n, cap),
        out_shape=pltpu.VMEM((rows, half), F32),
        in_specs=[hbm] * 7,
        out_specs=vmem,
        scratch_shapes=[
            pltpu.VMEM((rows, half), BF16),
            pltpu.VMEM((top, rows), jnp.int32),
            pltpu.VMEM((1, n), jnp.int32),
            pltpu.VMEM((top, rows), F32),
            dma((4,)),
            pltpu.VMEM((depth, hidden), BF16),
            pltpu.VMEM((depth, hidden), BF16),
            pltpu.VMEM((2, hidden, half), BF16),
            dma((3,)),
            dma, dma,
            dma((n,)), dma((n,)),
            dma((n,)), dma((n,)),
            dma((2,)), dma((2,)),
            dma((n,)), dma((n,)),
            pltpu.SemaphoreType.REGULAR((max(n // grid_width(n) + grid_width(n) - 3, 1),)),
            pltpu.VMEM((n, HEAD, wide), BF16),
            pltpu.VMEM((2, n, HEAD, wide), BF16),
            pltpu.VMEM((n, HEAD, wide), BF16),
            pltpu.VMEM((n, HEAD, wide), BF16),
        ] + [
            shape
            for cuts_at in wave_plans(n)
            for low, high in zip((0,) + cuts_at, cuts_at + (n,))
            for shape in (
                pltpu.VMEM((2, (high - low) * cap, hidden), BF16),
                pltpu.VMEM(((high - low) * cap, half), F32),
                pltpu.VMEM(((high - low) * cap, hidden), F32),
                pltpu.VMEM(((high - low) * cap, hidden), F32),
            )
        ],
        compiler_params=pltpu.CompilerParams(
            collective_id=0, has_side_effects=True, vmem_limit_bytes=60000 * 1024
        ),
    )(tokens, expert_ids.T, slot_expert.reshape(1, n), gate_values.T,
      gate_weight, up_weight, down_weight)
    return combined.astype(BF16)


def solution(mesh):
    return jax.shard_map(
        body,
        mesh=mesh,
        in_specs=(
            P(("groups", "ep"), "rep"),
            P(("groups", "ep"), None),
            P(("groups", "ep"), None),
            P(),
            P("ep", None, "rep"),
            P("ep", None, "rep"),
            P("ep", "rep", None),
        ),
        out_specs=P(("groups", "ep"), "rep"),
        check_vma=False,
    )
```

```python
import functools

import jax
import jax.numpy as jnp
from jax import lax
from jax.experimental import pallas as pl
from jax.experimental.pallas import tpu as pltpu
from jax.sharding import PartitionSpec as P

MESH = pl.DeviceIdType.MESH
F32 = jnp.float32
BF16 = jnp.bfloat16
HEAD = 8


def iota(shape, dim):
    return lax.broadcasted_iota(jnp.int32, shape, dim)


def repeat(low, high, step):
    if high - low <= 8:
        for i in reversed(range(low, high)):
            step(i)
    else:
        lax.fori_loop(0, high - low, lambda i, c: (step(high - 1 - i), c)[1], 0)


def mix(n, a, b):
    total, bit = 0, 1
    while bit < n:
        total = total + (a // bit + b // bit) % 2 * bit
        bit *= 2
    return total


def routing(ids, slots_row, ep, tail):
    top, rows = ids.shape
    n = slots_row.shape[1]
    at_row, at_col = iota((n, n), 0), iota((n, n), 1)
    slots_all = jnp.broadcast_to(slots_row, (n, n))
    slots_col = jnp.sum(jnp.where(at_row == at_col, slots_all, 0), axis=1, keepdims=True)
    same = slots_col == slots_all
    copies = jnp.sum(jnp.where(same, 1, 0), axis=1, keepdims=True)
    rank = jnp.sum(jnp.where(same & (at_col < at_row), 1, 0), axis=1, keepdims=True)
    want = jnp.zeros_like(copies)
    for c in range(2, 5):
        want = jnp.where(copies == c, lax.rem(ep, c), want)
    goes = jnp.zeros((n, rows), F32)
    for k in range(top):
        hit = (ids[k : k + 1, :] == slots_col) & (rank == want)
        goes = jnp.where(hit, 1.0, goes)
    before = jnp.where(iota((rows, rows), 0) < iota((rows, rows), 1), 1.0, 0.0)
    place = jnp.dot(goes, before, preferred_element_type=F32)
    r, s = iota((n * HEAD, n), 0), iota((n * HEAD, n), 1)
    m = place_of(n, ep, jnp.bitwise_xor(s, ep))
    mine = (r >= m * HEAD) & (r < m * HEAD + HEAD)
    spread = jnp.where(mine, 1.0, 0.0)
    index = jnp.sum(jnp.where(mine, r - m * HEAD, 0), axis=1, keepdims=True)
    experts = jnp.sum(
        jnp.where(mine, jnp.broadcast_to(slots_row, (n * HEAD, n)), 0), axis=1, keepdims=True
    )
    goes_r = jnp.dot(spread, goes, preferred_element_type=F32)
    place_r = jnp.dot(spread, place, preferred_element_type=F32)
    place_in = jnp.where(goes_r > 0.5, place_r, -1.0)
    heads = jnp.where(place_in == index.astype(F32), 1.0, 0.0)
    folds = []
    for q in range(HEAD // tail):
        wanted = jnp.where((index >= q * tail) & (index < q * tail + tail), index - q * tail + HEAD, -2)
        folds.append(jnp.where(place_in == wanted.astype(F32), 1.0, 0.0))
    return heads, folds, experts


def fold_width(half, tail):
    return (half * tail // HEAD + 127) // 128 * 128


def fold_cuts(half, tail):
    wide = fold_width(half, tail)
    return [(q * wide, min(wide, half - q * wide)) for q in range(HEAD // tail)]


def widen(piece, wide):
    short = wide - piece.shape[1]
    return jnp.concatenate([piece, jnp.zeros((piece.shape[0], short), piece.dtype)], 1) if short else piece


def place_of(n, ep, mask):
    width = grid_width(n)
    if n // width != 4:
        return mask
    row = ep // width
    inner = (row // 2 + row) % 2
    far = jnp.where(mask >= 2 * width, 1, 0)
    last = jnp.where(mask >= 3 * width, 1, 0)
    return mask + far * inner * (1 - 2 * last) * width


def kernel(n, cap, tok_hbm, ids_hbm, slots_hbm, gates_hbm, wg_hbm, wu_hbm, wd_hbm, out_ref,
           tok, ids_ref, slots_ref, gates_ref, in_sem,
           wg, wu, wd, w_sem, d_send, d_recv, s_send, s_recv, p_send, p_recv, r_send, r_recv, ready,
           send, x, res, ret, mine, theirs, mid):
    ep, rep = lax.axis_index("ep"), lax.axis_index("rep")
    other = 1 - rep
    rows, half = tok.shape
    tail = cap - HEAD
    cuts, wide = fold_cuts(half, tail), fold_width(half, tail)

    barrier = pltpu.get_barrier_semaphore()

    width = grid_width(n)
    height = n // width
    row, col = ep // width, ep % width
    beside = (
        (row > 0, ep - width), (row < height - 1, ep + width), (col > 0, ep - 1), (col < width - 1, ep + 1),
    )
    near_count = sum(jnp.where(there, 1, 0) for there, _ in beside)

    def tell(sem):
        for there, peer in beside:

            @pl.when(there)
            def _():
                pl.semaphore_signal(sem, inc=1, device_id={"ep": peer}, device_id_type=MESH)

    tell(barrier)
    pl.semaphore_signal(barrier, inc=1, device_id={"rep": other}, device_id_type=MESH)

    inputs = [
        pltpu.make_async_copy(ids_hbm, ids_ref, in_sem.at[0]),
        pltpu.make_async_copy(slots_hbm, slots_ref, in_sem.at[1]),
        pltpu.make_async_copy(tok_hbm, tok, in_sem.at[2]),
        pltpu.make_async_copy(gates_hbm, gates_ref, in_sem.at[3]),
    ]
    for copy in inputs:
        copy.start()
    def greet():
        pl.semaphore_wait(barrier, near_count + 1)
        if height + width > 3:
            tell(ready.at[0])

    pl.when(row == height - 1)(greet)
    def lines_of(side):
        return pl.ds(pl.multiple_of(side * half, 128), half)

    weights = [
        pltpu.make_async_copy(wg_hbm.at[0, lines_of(rep)], wg.at[rep], w_sem.at[0]),
        pltpu.make_async_copy(wu_hbm.at[0, lines_of(rep)], wu.at[rep], w_sem.at[1]),
        pltpu.make_async_copy(wd_hbm.at[0, :, lines_of(rep)], wd.at[rep], w_sem.at[2]),
    ]

    def lend(side):
        return [
            pltpu.make_async_remote_copy(
                src_ref=source, dst_ref=target.at[side], send_sem=d_send.at[i], recv_sem=d_recv.at[i],
                device_id={"rep": other}, device_id_type=MESH,
            )
            for i, (source, target) in enumerate((
                (wg_hbm.at[0, lines_of(other)], wg),
                (wu_hbm.at[0, lines_of(other)], wu),
                (wd_hbm.at[0, :, lines_of(other)], wd),
            ))
        ]

    inputs[0].wait()
    inputs[1].wait()
    heads, folds, experts = routing(ids_ref[...], slots_ref[...], ep, tail)
    inputs[2].wait()
    for copy in weights:
        copy.start()
    tokens = tok[...]

    def shape_up(block):
        return block.astype(BF16).reshape(block.shape[0] // HEAD, HEAD, block.shape[1])

    send[:, :, :half] = shape_up(jnp.dot(heads.astype(BF16), tokens, preferred_element_type=F32))
    folded = None
    for (at, size), pick in zip(cuts, folds):
        piece = jnp.dot(pick.astype(BF16), tokens[:, at : at + size], preferred_element_type=F32)
        piece = widen(piece, wide)
        folded = piece if folded is None else folded + piece
    send[:, :, half:] = shape_up(folded)
    inputs[3].wait()

    pl.when(row < height - 1)(greet)

    for copy in lend(rep):
        copy.start()

    def peer_of(p):
        mask = place_of(n, ep, p)
        peer = mix(n, ep, mask)
        return peer, place_of(n, peer, mask)

    def packet(p):
        peer, there = peer_of(p)
        return pltpu.make_async_remote_copy(
            src_ref=send.at[p], dst_ref=x.at[there], send_sem=s_send, recv_sem=s_recv,
            device_id={"ep": peer}, device_id_type=MESH,
        )

    def back(p):
        peer, there = peer_of(p)
        return pltpu.make_async_remote_copy(
            src_ref=res.at[p], dst_ref=ret.at[there], send_sem=r_send, recv_sem=r_recv,
            device_id={"ep": peer}, device_id_type=MESH,
        )

    others = pl.ds(1, n - 1)
    packets = pltpu.make_async_remote_copy(
        src_ref=send.at[others], dst_ref=x.at[others], send_sem=s_send, recv_sem=s_recv,
        device_id={"rep": other}, device_id_type=MESH,
    )
    backs = pltpu.make_async_remote_copy(
        src_ref=res.at[others], dst_ref=ret.at[others], send_sem=r_send, recv_sem=r_recv,
        device_id={"rep": other}, device_id_type=MESH,
    )

    def start_packet(p):
        packet(p).start()

    def distance(peer):
        there, place = peer // width, peer % width
        return jnp.where(there > row, there - row, row - there) + jnp.where(place > col, place - col, col - place)

    reach = height + width - 2
    for away in range(1, reach + 1):
        if away > 1:
            pl.semaphore_wait(ready.at[away - 2], near_count)
        if 1 < away < reach:
            tell(ready.at[away - 1])
        if n <= 8:
            for p in range(1, n):
                pl.when(distance(peer_of(p)[0]) == away)(functools.partial(start_packet, p))
    if n > 8:
        repeat(1, n, start_packet)
    x[0] = send[0]
    over = (((0,), (0,)), ((), ()))

    def tails(block):
        rows_of = [
            block[:, q * tail : q * tail + tail, :size].reshape(n * tail, size) for q, (_, size) in enumerate(cuts)
        ]
        return jnp.concatenate(rows_of, axis=1)

    hidden = wd.shape[1]
    parts, span = mine.shape[0], mine.shape[3]

    def exchange(c):
        return pltpu.make_async_remote_copy(
            src_ref=mine.at[c], dst_ref=theirs.at[c], send_sem=p_send.at[c], recv_sem=p_recv.at[c],
            device_id={"rep": other}, device_id_type=MESH,
        )

    packets.wait_recv()
    weights[0].wait()
    weights[1].wait()
    lent = lend(other)
    lent[0].wait_recv()
    lent[1].wait_recv()
    upper = x[:, :, :half].reshape(n * HEAD, half)
    block = jnp.concatenate([upper, tails(x[:, :, half:])], axis=0)
    for c in range(parts):
        side, at = c * span // hidden, c * span % hidden
        mine[c, 0] = jnp.dot(block, wg[side, :, at : at + span], preferred_element_type=F32)
        mine[c, 1] = jnp.dot(block, wu[side, :, at : at + span], preferred_element_type=F32)
        exchange(c).start()

    weights[2].wait()
    lent[2].wait_recv()

    def hidden_part(c):
        exchange(c).wait_recv()
        gate = mine[c, 0] + theirs[c, 0]
        up = mine[c, 1] + theirs[c, 1]
        return ((gate / (1.0 + jnp.exp(-gate))) * up).astype(BF16)

    for c in range(parts):
        side, at = c * span // hidden, c * span % hidden
        more = jnp.dot(hidden_part(c), wd[side, at : at + span, :], preferred_element_type=F32)
        if c == 0:
            mid[...] = more
        elif c < parts - 1:
            mid[...] += more
    result = mid[...] + more
    split = n * HEAD
    res[:, :, :half] = shape_up(result[:split])
    last = result[split:].astype(BF16)
    for q, (at, size) in enumerate(cuts):
        piece = widen(last[:, at : at + size], wide).reshape(n, tail, wide)
        res[:, q * tail : q * tail + tail, half:] = piece
    repeat(1, n, lambda p: back(p).start())
    ret[0] = res[0]
    for copy in lend(rep):
        copy.wait_send()
    for c in range(parts):
        exchange(c).wait_send()
    packets.wait_send()
    backs.wait_recv()
    ids = ids_ref[...]
    gates = gates_ref[...]
    all_heads = ret[:, :, :half].reshape(n * HEAD, half)
    all_folds = ret[:, :, half:].reshape(n * HEAD, wide)
    diagonal = iota((rows, rows), 0) == iota((rows, rows), 1)
    total = None
    for k in range(ids.shape[0]):
        named = ids[k : k + 1, :] == experts
        hit = jnp.where(named, heads, 0.0).astype(BF16)
        got = lax.dot_general(hit, all_heads, over, preferred_element_type=F32)
        pieces = []
        for (_, size), pick in zip(cuts, folds):
            hit = jnp.where(named, pick, 0.0).astype(BF16)
            pieces.append(lax.dot_general(hit, all_folds[:, :size], over, preferred_element_type=F32))
        got = got + jnp.concatenate(pieces, axis=1)
        line = jnp.broadcast_to(gates[k : k + 1, :], (rows, rows))
        column = jnp.sum(jnp.where(diagonal, line, 0.0), axis=1, keepdims=True)
        total = got * column if total is None else total + got * column
    out_ref[...] = total

    backs.wait_send()


def grid_width(n):
    width = 1
    while width * width * 4 <= n:
        width *= 2
    return width


def body(tokens, expert_ids, gate_values, slot_expert, gate_weight, up_weight, down_weight):
    rows, top = expert_ids.shape
    half = tokens.shape[1]
    n = slot_expert.shape[0]
    experts = n // 2
    cap = rows * top * 5 // (4 * experts)
    tail = cap - HEAD
    hidden = gate_weight.shape[2]
    span = hidden
    parts = 2 * hidden // span
    vmem = pl.BlockSpec(memory_space=pltpu.VMEM)
    hbm = pl.BlockSpec(memory_space=pl.ANY)
    dma = pltpu.SemaphoreType.DMA
    wide = half + fold_width(half, tail)

    combined = pl.pallas_call(
        functools.partial(kernel, n, cap),
        out_shape=pltpu.VMEM((rows, half), F32),
        in_specs=[hbm] * 7,
        out_specs=vmem,
        scratch_shapes=[
            pltpu.VMEM((rows, half), BF16),
            pltpu.VMEM((top, rows), jnp.int32),
            pltpu.VMEM((1, n), jnp.int32),
            pltpu.VMEM((top, rows), F32),
            dma((4,)),
            pltpu.VMEM((2, half, hidden), BF16),
            pltpu.VMEM((2, half, hidden), BF16),
            pltpu.VMEM((2, hidden, half), BF16),
            dma((3,)), dma((3,)), dma((3,)),
            dma, dma,
            dma((parts,)), dma((parts,)),
            dma, dma,
            pltpu.SemaphoreType.REGULAR((max(n // grid_width(n) + grid_width(n) - 3, 1),)),
            pltpu.VMEM((n, HEAD, wide), BF16),
            pltpu.VMEM((n, HEAD, wide), BF16),
            pltpu.VMEM((n, HEAD, wide), BF16),
            pltpu.VMEM((n, HEAD, wide), BF16),
            pltpu.VMEM((parts, 2, n * cap, span), F32),
            pltpu.VMEM((parts, 2, n * cap, span), F32),
            pltpu.VMEM((n * cap, half), F32),
        ],
        compiler_params=pltpu.CompilerParams(
            collective_id=0, has_side_effects=True, vmem_limit_bytes=60000 * 1024
        ),
    )(tokens, expert_ids.T, slot_expert.reshape(1, n), gate_values.T,
      gate_weight, up_weight, down_weight)
    return combined.astype(BF16)


def solution(mesh):
    return jax.shard_map(
        body,
        mesh=mesh,
        in_specs=(
            P(("groups", "ep"), "rep"),
            P(("groups", "ep"), None),
            P(("groups", "ep"), None),
            P(),
            P("ep", None, "rep"),
            P("ep", None, "rep"),
            P("ep", "rep", None),
        ),
        out_specs=P(("groups", "ep"), "rep"),
        check_vma=False,
    )
```

```python
import functools

import jax
import jax.numpy as jnp
from jax import lax
from jax.experimental import pallas as pl
from jax.experimental.pallas import tpu as pltpu
from jax.sharding import PartitionSpec as P

MESH = pl.DeviceIdType.MESH
F32 = jnp.float32
BF16 = jnp.bfloat16
HEAD = 8


def iota(shape, dim):
    return lax.broadcasted_iota(jnp.int32, shape, dim)


def repeat(low, high, step):
    if high - low <= 8:
        for i in reversed(range(low, high)):
            step(i)
    else:
        lax.fori_loop(0, high - low, lambda i, c: (step(high - 1 - i), c)[1], 0)


def mix(n, a, b):
    total, bit = 0, 1
    while bit < n:
        total = total + (a // bit + b // bit) % 2 * bit
        bit *= 2
    return total


def groups_of(n):
    return 2 if (n, grid_width(n)) == (8, 2) else 1


def routing(ids, slots_row, ep, tail):
    top, nodes = ids.shape
    n = slots_row.shape[1]
    at_row, at_col = iota((n, n), 0), iota((n, n), 1)
    slots_all = jnp.broadcast_to(slots_row, (n, n))
    slots_col = jnp.sum(jnp.where(at_row == at_col, slots_all, 0), axis=1, keepdims=True)
    same = slots_col == slots_all
    copies = jnp.sum(jnp.where(same, 1, 0), axis=1, keepdims=True)
    rank = jnp.sum(jnp.where(same & (at_col < at_row), 1, 0), axis=1, keepdims=True)
    want = jnp.zeros_like(copies)
    for c in range(2, 5):
        want = jnp.where(copies == c, lax.rem(ep, c), want)
    goes = jnp.zeros((n, nodes), F32)
    for k in range(top):
        hit = (ids[k : k + 1, :] == slots_col) & (rank == want)
        goes = jnp.where(hit, 1.0, goes)
    before = jnp.where(iota((nodes, nodes), 0) < iota((nodes, nodes), 1), 1.0, 0.0)
    place = jnp.dot(goes, before, preferred_element_type=F32)
    size = n // groups_of(n)
    shape = (n * (HEAD + tail), n)
    r, s = iota(shape, 0), iota(shape, 1)
    m = place_of(n, ep, jnp.bitwise_xor(s, ep))
    later = jnp.where(m >= size, 1, 0)
    base, inside = later * (size * (HEAD + tail)), m - later * size
    head = r - (base + inside * HEAD)
    foot = r - (base + size * HEAD + inside * tail)
    in_head = (head >= 0) & (head < HEAD)
    in_foot = (foot >= 0) & (foot < tail)
    mine = in_head | in_foot
    spread = jnp.where(mine, 1.0, 0.0)
    index = jnp.sum(jnp.where(in_head, head, jnp.where(in_foot, foot + HEAD, 0)), axis=1, keepdims=True)
    experts = jnp.sum(jnp.where(mine, jnp.broadcast_to(slots_row, shape), 0), axis=1, keepdims=True)
    goes_r = jnp.dot(spread, goes, preferred_element_type=F32)
    place_r = jnp.dot(spread, place, preferred_element_type=F32)
    place_in = jnp.where(goes_r > 0.5, place_r, -1.0)
    return jnp.where(place_in == index.astype(F32), 1.0, 0.0), experts


def place_of(n, ep, mask):
    width = grid_width(n)
    if n // width != 4:
        return mask
    row = ep // width
    inner = (row // 2 + row) % 2
    far = jnp.where(mask >= 2 * width, 1, 0)
    last = jnp.where(mask >= 3 * width, 1, 0)
    return mask + far * inner * (1 - 2 * last) * width


def kernel(n, cap, tok_hbm, ids_hbm, slots_hbm, gates_hbm, wg_hbm, wu_hbm, wd_hbm, out_ref,
           tok, ids_ref, slots_ref, gates_ref, in_sem,
           wg, wu, wd, w_sem, d_send, d_recv, s_send, s_recv, p_send, p_recv, r_send, r_recv, ready, gate,
           send, x, res, ret, mine, theirs, mid):
    ep, rep = lax.axis_index("ep"), lax.axis_index("rep")
    other = 1 - rep
    nodes, half = tok.shape
    tail = cap - HEAD
    size = n // groups_of(n)
    hidden = wd.shape[1]
    parts, span = mine.shape[0], mine.shape[3]

    barrier = pltpu.get_barrier_semaphore()

    width = grid_width(n)
    height = n // width
    row, col = ep // width, ep % width
    beside = (
        (row > 0, ep - width), (row < height - 1, ep + width), (col > 0, ep - 1), (col < width - 1, ep + 1),
    )
    near_count = sum(jnp.where(there, 1, 0) for there, _ in beside)
    reach = height + width - 2

    def tell(sem):
        for there, peer in beside:

            @pl.when(there)
            def _():
                pl.semaphore_signal(sem, inc=1, device_id={"ep": peer}, device_id_type=MESH)

    tell(barrier)
    pl.semaphore_signal(barrier, inc=1, device_id={"rep": other}, device_id_type=MESH)

    inputs = [
        pltpu.make_async_copy(ids_hbm, ids_ref, in_sem.at[0]),
        pltpu.make_async_copy(slots_hbm, slots_ref, in_sem.at[1]),
        pltpu.make_async_copy(tok_hbm, tok, in_sem.at[2]),
        pltpu.make_async_copy(gates_hbm, gates_ref, in_sem.at[3]),
    ]
    for copy in inputs:
        copy.start()

    def lines_of(side):
        return pl.ds(pl.multiple_of(side * half, 128), half)

    weights = [
        pltpu.make_async_copy(wg_hbm.at[0, lines_of(rep)], wg.at[rep], w_sem.at[0]),
        pltpu.make_async_copy(wu_hbm.at[0, lines_of(rep)], wu.at[rep], w_sem.at[1]),
        pltpu.make_async_copy(wd_hbm.at[0, :, lines_of(rep)], wd.at[rep], w_sem.at[2]),
    ]

    def lend(side):
        return [
            pltpu.make_async_remote_copy(
                src_ref=source, dst_ref=target.at[side], send_sem=d_send.at[i], recv_sem=d_recv.at[i],
                device_id={"rep": other}, device_id_type=MESH,
            )
            for i, (source, target) in enumerate((
                (wg_hbm.at[0, lines_of(other)], wg),
                (wu_hbm.at[0, lines_of(other)], wu),
                (wd_hbm.at[0, :, lines_of(other)], wd),
            ))
        ]

    def greet():
        pl.semaphore_wait(barrier, near_count + 1)
        if reach > 1:
            tell(ready.at[0])

    pl.when(row == height - 1)(greet)
    inputs[0].wait()
    inputs[1].wait()
    pick, experts = routing(ids_ref[...], slots_ref[...], ep, tail)
    inputs[2].wait()
    for copy in weights:
        copy.start()
    send[...] = jnp.dot(pick.astype(BF16), tok[...], preferred_element_type=F32).astype(BF16)
    inputs[3].wait()
    pl.when(row < height - 1)(greet)
    for copy in lend(rep):
        copy.start()

    def peer_of(p):
        mask = place_of(n, ep, p)
        peer = mix(n, ep, mask)
        return peer, place_of(n, peer, mask)

    held = width if groups_of(n) == 2 else 0
    urgent = n - 2 * held
    send_groups = ((1, urgent), (urgent, n - held), (n - held, n)) if held else ((1, n),)
    recv_groups = ((0, size), (size, n)) if groups_of(n) == 2 else ((0, n),)

    def rows_of(p):
        group = p // size
        base, inside = group * (size * cap), p % size
        return (
            pl.ds(pl.multiple_of(base + inside * HEAD, HEAD), HEAD),
            pl.ds(pl.multiple_of(base + size * HEAD + inside * tail, tail), tail),
        )

    def copies(source, target, p, send_sem, recv_sem):
        peer, there = peer_of(p)
        return [
            pltpu.make_async_remote_copy(
                src_ref=source.at[here], dst_ref=target.at[away], send_sem=send_sem,
                recv_sem=recv_sem.at[there // size], device_id={"ep": peer}, device_id_type=MESH,
            )
            for here, away in zip(rows_of(p), rows_of(there))
        ]

    def start_packet(p, group=0):
        for copy in copies(send, x, p, s_send.at[group], s_recv):
            copy.start()

    def start_back(p):
        for copy in copies(res, ret, p, r_send, r_recv):
            copy.start()

    def bytes_of(source, target, rows, columns, send_sem, recv_sem):
        some = (pl.ds(0, rows), pl.ds(0, columns))
        return pltpu.make_async_remote_copy(
            src_ref=source.at[some], dst_ref=target.at[some], send_sem=send_sem, recv_sem=recv_sem,
            device_id={"rep": other}, device_id_type=MESH,
        )

    def drain(source, target, places, send_sem):
        blocks = [(4 * cap, half)] * (places // 4) + [(4 * cap, half // 2)] * (places // 2 % 2)
        blocks += [(HEAD, half), (tail, half)] * (places % 2)
        for rows, columns in blocks:
            bytes_of(source, target, rows, columns, send_sem, s_recv.at[0]).wait_send()

    def sent(group):
        low, high = send_groups[group]
        drain(send, x, high - low, s_send.at[group])

    def received(group):
        bytes_of(send, x, size * cap, half, s_send.at[0], s_recv.at[group]).wait_recv()

    def returned(group):
        bytes_of(res, ret, size * cap, half, r_send, r_recv.at[group]).wait_recv()

    def keep(source, target, sem):
        for here in rows_of(0):
            pltpu.make_async_copy(source.at[here], target.at[here], sem.at[0]).start()

    def distance(peer):
        there, place = peer // width, peer % width
        return jnp.where(there > row, there - row, row - there) + jnp.where(place > col, place - col, col - place)

    for away in range(1, reach + 1):
        if away > 1:
            pl.semaphore_wait(ready.at[away - 2], near_count)
        if 1 < away < reach:
            tell(ready.at[away - 1])
        if n <= 8:
            for p in range(1, n):
                now = distance(peer_of(p)[0]) == away
                group = [p >= low and p < high for low, high in send_groups].index(True)
                if held and group == 2:
                    now = now & (rep == 0)
                pl.when(now)(functools.partial(start_packet, p, group))
    if n > 8:
        repeat(1, n, start_packet)
    keep(send, x, s_recv)
    if held:

        @pl.when(rep == 0)
        def _():
            sent(1)
            pl.semaphore_signal(gate, inc=1, device_id={"rep": other}, device_id_type=MESH)

        @pl.when(rep == 1)
        def _():
            pl.semaphore_wait(gate, 1)
            for p in range(n - held, n):
                start_packet(p, 2)
            sent(1)

    over = (((0,), (0,)), ((), ()))

    def exchange(w, c, lines):
        return pltpu.make_async_remote_copy(
            src_ref=mine.at[c, :, lines], dst_ref=theirs.at[c, :, lines],
            send_sem=p_send.at[w], recv_sem=p_recv.at[w, c],
            device_id={"rep": other}, device_id_type=MESH,
        )

    def wave(w, low, high):
        first, count = low * cap, (high - low) * cap
        lines = pl.ds(first, count)
        for group, (start, stop) in enumerate(recv_groups):
            if low < stop and start < high:
                received(group)
        if w == 0:
            weights[0].wait()
            weights[1].wait()
            lent = lend(other)
            lent[0].wait_recv()
            lent[1].wait_recv()
        for c in range(parts):
            side, at = c * span // hidden, c * span % hidden
            block = x[lines, :]
            mine[c, 0, lines, :] = jnp.dot(block, wg[side, :, at : at + span], preferred_element_type=F32)
            mine[c, 1, lines, :] = jnp.dot(block, wu[side, :, at : at + span], preferred_element_type=F32)
            exchange(w, c, lines).start()
        if w == 0:
            weights[2].wait()
            lent[2].wait_recv()
        for c in range(parts):
            side, at = c * span // hidden, c * span % hidden
            exchange(w, c, lines).wait_recv()
            g = mine[c, 0, lines, :] + theirs[c, 0, lines, :]
            u = mine[c, 1, lines, :] + theirs[c, 1, lines, :]
            value = ((g / (1.0 + jnp.exp(-g))) * u).astype(BF16)
            more = jnp.dot(value, wd[side, at : at + span, :], preferred_element_type=F32)
            if c == 0:
                mid[lines, :] = more
            elif c < parts - 1:
                mid[lines, :] += more
            else:
                res[lines, :] = (mid[lines, :] + more).astype(BF16)
        repeat(max(low, 1), high, start_back)
        for c in range(parts):
            exchange(w, c, lines).wait_send()

    def run(plan):
        for w, (low, high) in enumerate(plan):
            wave(w, low, high)

    if groups_of(n) == 2:
        pl.when(row == 0)(functools.partial(run, ((0, size), (size, n))))
        pl.when(row > 0)(functools.partial(run, ((0, n),)))
    else:
        run(((0, n),))

    keep(res, ret, r_recv)
    for copy in lend(rep):
        copy.wait_send()
    for group in range(len(send_groups)):
        if not (held and group == 1):
            sent(group)

    ids = ids_ref[...]
    gates = gates_ref[...]
    diagonal = iota((nodes, nodes), 0) == iota((nodes, nodes), 1)
    combined = None
    for group in range(len(recv_groups)):
        returned(group)
        lines = slice(group * size * cap, (group + 1) * size * cap)
        block = ret[lines, :]
        for k in range(ids.shape[0]):
            hit = jnp.where(ids[k : k + 1, :] == experts[lines], pick[lines], 0.0).astype(BF16)
            got = lax.dot_general(hit, block, over, preferred_element_type=F32)
            line = jnp.broadcast_to(gates[k : k + 1, :], (nodes, nodes))
            column = jnp.sum(jnp.where(diagonal, line, 0.0), axis=1, keepdims=True)
            combined = got * column if combined is None else combined + got * column
    out_ref[...] = combined
    drain(res, ret, n - 1, r_send)


def grid_width(n):
    width = 1
    while width * width * 4 <= n:
        width *= 2
    return width


def body(tokens, expert_ids, gate_values, slot_expert, gate_weight, up_weight, down_weight):
    nodes, top = expert_ids.shape
    half = tokens.shape[1]
    n = slot_expert.shape[0]
    cap = nodes * top * 5 // (4 * (n // 2))
    hidden = gate_weight.shape[2]
    span = min(hidden, 256)
    parts = 2 * hidden // span
    groups = groups_of(n)
    hbm = pl.BlockSpec(memory_space=pl.ANY)
    dma = pltpu.SemaphoreType.DMA
    regular = pltpu.SemaphoreType.REGULAR

    combined = pl.pallas_call(
        functools.partial(kernel, n, cap),
        out_shape=pltpu.VMEM((nodes, half), F32),
        in_specs=[hbm] * 7,
        out_specs=pl.BlockSpec(memory_space=pltpu.VMEM),
        scratch_shapes=[
            pltpu.VMEM((nodes, half), BF16),
            pltpu.VMEM((top, nodes), jnp.int32),
            pltpu.VMEM((1, n), jnp.int32),
            pltpu.VMEM((top, nodes), F32),
            dma((4,)),
            pltpu.VMEM((2, half, hidden), BF16),
            pltpu.VMEM((2, half, hidden), BF16),
            pltpu.VMEM((2, hidden, half), BF16),
            dma((3,)), dma((3,)), dma((3,)),
            dma((2 * groups - 1,)), dma((groups,)),
            dma((groups,)), dma((groups, parts)),
            dma, dma((groups,)),
            regular((max(n // grid_width(n) + grid_width(n) - 3, 1),)),
            regular,
            pltpu.VMEM((n * cap, half), BF16),
            pltpu.VMEM((n * cap, half), BF16),
            pltpu.VMEM((n * cap, half), BF16),
            pltpu.VMEM((n * cap, half), BF16),
            pltpu.VMEM((parts, 2, n * cap, span), F32),
            pltpu.VMEM((parts, 2, n * cap, span), F32),
            pltpu.VMEM((n * cap, half), F32),
        ],
        compiler_params=pltpu.CompilerParams(
            collective_id=0, has_side_effects=True, vmem_limit_bytes=60000 * 1024
        ),
    )(tokens, expert_ids.T, slot_expert.reshape(1, n), gate_values.T,
      gate_weight, up_weight, down_weight)
    return combined.astype(BF16)


def solution(mesh):
    return jax.shard_map(
        body,
        mesh=mesh,
        in_specs=(
            P(("groups", "ep"), "rep"),
            P(("groups", "ep"), None),
            P(("groups", "ep"), None),
            P(),
            P("ep", None, "rep"),
            P("ep", None, "rep"),
            P("ep", "rep", None),
        ),
        out_specs=P(("groups", "ep"), "rep"),
        check_vma=False,
    )
```

```python
import functools

import jax
import jax.numpy as jnp
from jax import lax
from jax.experimental import pallas as pl
from jax.experimental.pallas import tpu as pltpu
from jax.sharding import PartitionSpec as P

MESH = pl.DeviceIdType.MESH
F32 = jnp.float32
BF16 = jnp.bfloat16
HEAD = 8


def iota(shape, dim):
    return lax.broadcasted_iota(jnp.int32, shape, dim)


def repeat(low, high, step):
    if high - low <= 8:
        for i in reversed(range(low, high)):
            step(i)
    else:
        lax.fori_loop(0, high - low, lambda i, c: (step(high - 1 - i), c)[1], 0)


def mix(n, a, b):
    total, bit = 0, 1
    while bit < n:
        total = total + (a // bit + b // bit) % 2 * bit
        bit *= 2
    return total


def groups_of(n):
    return 2 if (n, grid_width(n)) == (8, 2) else 1


def routing(ids, slots_row, ep, tail):
    top, nodes = ids.shape
    n = slots_row.shape[1]
    at_row, at_col = iota((n, n), 0), iota((n, n), 1)
    slots_all = jnp.broadcast_to(slots_row, (n, n))
    slots_col = jnp.sum(jnp.where(at_row == at_col, slots_all, 0), axis=1, keepdims=True)
    same = slots_col == slots_all
    copies = jnp.sum(jnp.where(same, 1, 0), axis=1, keepdims=True)
    rank = jnp.sum(jnp.where(same & (at_col < at_row), 1, 0), axis=1, keepdims=True)
    want = jnp.zeros_like(copies)
    for c in range(2, 5):
        want = jnp.where(copies == c, lax.rem(ep, c), want)
    goes = jnp.zeros((n, nodes), F32)
    for k in range(top):
        hit = (ids[k : k + 1, :] == slots_col) & (rank == want)
        goes = jnp.where(hit, 1.0, goes)
    before = jnp.where(iota((nodes, nodes), 0) < iota((nodes, nodes), 1), 1.0, 0.0)
    place = jnp.dot(goes, before, preferred_element_type=F32)
    size = n // groups_of(n)
    shape = (n * (HEAD + tail), n)
    r, s = iota(shape, 0), iota(shape, 1)
    m = place_of(n, ep, jnp.bitwise_xor(s, ep))
    later = jnp.where(m >= size, 1, 0)
    base, inside = later * (size * (HEAD + tail)), m - later * size
    head = r - (base + inside * HEAD)
    foot = r - (base + size * HEAD + inside * tail)
    in_head = (head >= 0) & (head < HEAD)
    in_foot = (foot >= 0) & (foot < tail)
    mine = in_head | in_foot
    spread = jnp.where(mine, 1.0, 0.0)
    index = jnp.sum(jnp.where(in_head, head, jnp.where(in_foot, foot + HEAD, 0)), axis=1, keepdims=True)
    experts = jnp.sum(jnp.where(mine, jnp.broadcast_to(slots_row, shape), 0), axis=1, keepdims=True)
    goes_r = jnp.dot(spread, goes, preferred_element_type=F32)
    place_r = jnp.dot(spread, place, preferred_element_type=F32)
    place_in = jnp.where(goes_r > 0.5, place_r, -1.0)
    return jnp.where(place_in == index.astype(F32), 1.0, 0.0), experts


def place_of(n, ep, mask):
    width = grid_width(n)
    if n // width != 4:
        return mask
    row = ep // width
    inner = (row // 2 + row) % 2
    far = jnp.where(mask >= 2 * width, 1, 0)
    last = jnp.where(mask >= 3 * width, 1, 0)
    return mask + far * inner * (1 - 2 * last) * width


def kernel(n, cap, tok_hbm, ids_hbm, slots_hbm, gates_hbm, wg_hbm, wu_hbm, wd_hbm, out_ref,
           tok, ids_ref, slots_ref, gates_ref, in_sem,
           wg, wu, wd, d_send, d_recv, s_send, s_recv, p_send, p_recv, r_send, r_recv, ready, gate, turn,
           send, x, res, ret, mine, theirs, mid, *spare):
    ep, rep = lax.axis_index("ep"), lax.axis_index("rep")
    other = 1 - rep
    nodes, half = tok.shape
    tail = cap - HEAD
    size = n // groups_of(n)
    hidden = wd.shape[1]
    parts, span = mine.shape[0], mine.shape[3]

    barrier = pltpu.get_barrier_semaphore()

    width = grid_width(n)
    height = n // width
    row, col = ep // width, ep % width
    beside = (
        (row > 0, ep - width), (row < height - 1, ep + width), (col > 0, ep - 1), (col < width - 1, ep + 1),
    )
    near_count = sum(jnp.where(there, 1, 0) for there, _ in beside)
    reach = height + width - 2

    def tell(sem):
        for there, peer in beside:

            @pl.when(there)
            def _():
                pl.semaphore_signal(sem, inc=1, device_id={"ep": peer}, device_id_type=MESH)

    tell(barrier)
    pl.semaphore_signal(barrier, inc=1, device_id={"rep": other}, device_id_type=MESH)

    inputs = [
        pltpu.make_async_copy(ids_hbm, ids_ref, in_sem.at[0]),
        pltpu.make_async_copy(slots_hbm, slots_ref, in_sem.at[1]),
        pltpu.make_async_copy(tok_hbm, tok, in_sem.at[2]),
        pltpu.make_async_copy(gates_hbm, gates_ref, in_sem.at[3]),
    ]
    for copy in inputs:
        copy.start()

    def lines_of(side):
        return pl.ds(pl.multiple_of(side * half, 128), half)

    weights = [
        pltpu.make_async_copy(wg_hbm.at[0, lines_of(rep)], wg.at[rep], in_sem.at[0]),
        pltpu.make_async_copy(wu_hbm.at[0, lines_of(rep)], wu.at[rep], in_sem.at[1]),
        pltpu.make_async_copy(wd_hbm.at[0, :, lines_of(rep)], wd.at[rep], in_sem.at[2]),
    ]

    def lend(side):
        return [
            pltpu.make_async_remote_copy(
                src_ref=source, dst_ref=target.at[side], send_sem=d_send.at[i], recv_sem=d_recv.at[i],
                device_id={"rep": other}, device_id_type=MESH,
            )
            for i, (source, target) in enumerate((
                (wg_hbm.at[0, lines_of(other)], wg),
                (wu_hbm.at[0, lines_of(other)], wu),
                (wd_hbm.at[0, :, lines_of(other)], wd),
            ))
        ]

    def greet():
        pl.semaphore_wait(barrier, near_count + 1)
        if reach > 1:
            tell(ready.at[0])

    pl.when(row == height - 1)(greet)
    inputs[0].wait()
    inputs[1].wait()
    pick, experts = routing(ids_ref[...], slots_ref[...], ep, tail)
    inputs[2].wait()
    for copy in weights:
        copy.start()
    send[...] = jnp.dot(pick.astype(BF16), tok[...], preferred_element_type=F32).astype(BF16)
    inputs[3].wait()
    pl.when(row < height - 1)(greet)
    for copy in lend(rep):
        copy.start()

    def peer_of(p):
        mask = place_of(n, ep, p)
        peer = mix(n, ep, mask)
        return peer, place_of(n, peer, mask)

    held = width if groups_of(n) == 2 else 0
    urgent = n - 2 * held
    send_groups = ((1, urgent), (urgent, n - held), (n - held, n)) if held else ((1, n),)
    recv_groups = ((0, size), (size, n)) if groups_of(n) == 2 else ((0, n),)

    def rows_of(p):
        group = p // size
        base, inside = group * (size * cap), p % size
        return (
            pl.ds(pl.multiple_of(base + inside * HEAD, HEAD), HEAD),
            pl.ds(pl.multiple_of(base + size * HEAD + inside * tail, tail), tail),
        )

    def copies(source, target, p, send_sem, recv_sem):
        peer, there = peer_of(p)
        return [
            pltpu.make_async_remote_copy(
                src_ref=source.at[here], dst_ref=target.at[away], send_sem=send_sem,
                recv_sem=recv_sem.at[there // size], device_id={"ep": peer}, device_id_type=MESH,
            )
            for here, away in zip(rows_of(p), rows_of(there))
        ]

    def start_packet(p, group=0):
        for copy in copies(send, x, p, s_send.at[group], s_recv):
            copy.start()

    def start_back(p, group=0):
        for copy in copies(res, ret, p, r_send.at[group], r_recv):
            copy.start()

    def bytes_of(source, target, rows, columns, send_sem, recv_sem):
        some = (pl.ds(0, rows), pl.ds(0, columns))
        return pltpu.make_async_remote_copy(
            src_ref=source.at[some], dst_ref=target.at[some], send_sem=send_sem, recv_sem=recv_sem,
            device_id={"rep": other}, device_id_type=MESH,
        )

    def drain(source, target, places, send_sem):
        blocks = [(4 * cap, half)] * (places // 4) + [(4 * cap, half // 2)] * (places // 2 % 2)
        blocks += [(HEAD, half), (tail, half)] * (places % 2)
        for rows, columns in blocks:
            bytes_of(source, target, rows, columns, send_sem, s_recv.at[0]).wait_send()

    def sent(group):
        low, high = send_groups[group]
        drain(send, x, high - low, s_send.at[group])

    def received(group):
        bytes_of(send, x, size * cap, half, s_send.at[0], s_recv.at[group]).wait_recv()

    def returned(group):
        bytes_of(res, ret, size * cap, half, r_send.at[0], r_recv.at[group]).wait_recv()

    def keep(source, target, sem):
        for here in rows_of(0):
            pltpu.make_async_copy(source.at[here], target.at[here], sem.at[0]).start()

    def distance(peer):
        there, place = peer // width, peer % width
        return jnp.where(there > row, there - row, row - there) + jnp.where(place > col, place - col, col - place)

    outer = (row // 2 + row) % 2 == 0
    for away in range(1, reach + 1):
        if held and away == reach:

            @pl.when(rep == 1)
            def _():
                pl.semaphore_wait(ready.at[away - 2], near_count)
                tell(ready.at[away - 1])

            @pl.when(rep == 0)
            def _():
                pl.semaphore_wait(gate, 1)

        elif away > 1:
            pl.semaphore_wait(ready.at[away - 2], near_count)
        if held and away == reach - 1:
            pl.when(rep == 1)(lambda: tell(ready.at[away - 1]))
        elif 1 < away < reach:
            tell(ready.at[away - 1])
        if n <= 8:
            for p in range(1, n):
                now = distance(peer_of(p)[0]) == away
                group = [p >= low and p < high for low, high in send_groups].index(True)
                if held and group == 2:
                    now = now & (rep == 0)
                pl.when(now)(functools.partial(start_packet, p, group))
        if held and away == reach - 1:

            @pl.when((rep == 0) & jnp.logical_not(outer))
            def _():
                sent(1)
                pl.semaphore_signal(gate, inc=1, device_id={"rep": other}, device_id_type=MESH)

    if n > 8:
        repeat(1, n, start_packet)
    keep(send, x, s_recv)
    if held:

        @pl.when(rep == 1)
        def _():
            pl.semaphore_wait(ready.at[reach - 1], near_count)
            pl.semaphore_signal(gate, inc=1, device_id={"rep": other}, device_id_type=MESH)
            pl.when(jnp.logical_not(outer))(lambda: pl.semaphore_wait(gate, 1))
            for p in range(n - held, n):
                start_packet(p, 2)
            sent(1)

        @pl.when((rep == 0) & outer)
        def _():
            sent(1)

    over = (((0,), (0,)), ((), ()))

    def exchange(w, c, lines):
        return pltpu.make_async_remote_copy(
            src_ref=mine.at[c, :, lines], dst_ref=theirs.at[c, :, lines],
            send_sem=p_send, recv_sem=p_recv.at[w, c],
            device_id={"rep": other}, device_id_type=MESH,
        )

    def give_back(low, high):
        if not held or high < n:
            repeat(max(low, 1), high, start_back)
            return
        for p in reversed(range(n - held, n)):
            start_back(p, 1)
        upper = row == height - 1

        @pl.when(upper & (rep == 1))
        def _():
            pl.semaphore_wait(turn, 1)

        for p in reversed(range(max(low, 1), n - held)):
            start_back(p)

        drain(res, ret, held, r_send.at[1])

        @pl.when(upper & (rep == 0))
        def _():
            pl.semaphore_signal(turn, inc=1, device_id={"rep": other}, device_id_type=MESH)

    def wave(w, low, high):
        first, count = low * cap, (high - low) * cap
        lines = pl.ds(first, count)
        for group, (start, stop) in enumerate(recv_groups):
            if low < stop and start < high:
                received(group)
        if w == 0:
            weights[0].wait()
            weights[1].wait()
            lent = lend(other)
            lent[0].wait_recv()
            lent[1].wait_recv()
        for c in range(parts):
            side, at = c * span // hidden, c * span % hidden
            block = x[lines, :]
            for i, weight in enumerate((wg, wu)):
                mine[c, i, lines, :] = jnp.dot(
                    block, weight[side, :, at : at + span], preferred_element_type=F32
                )
            exchange(w, c, lines).start()
        if w == 0:
            weights[2].wait()
            lent[2].wait_recv()
        for c in range(parts):
            side, at = c * span // hidden, c * span % hidden
            exchange(w, c, lines).wait_recv()
            g = mine[c, 0, lines, :] + theirs[c, 0, lines, :]
            u = mine[c, 1, lines, :] + theirs[c, 1, lines, :]
            value = ((g / (1.0 + jnp.exp(-g))) * u).astype(BF16)
            more = jnp.dot(value, wd[side, at : at + span, :], preferred_element_type=F32)
            if c == 0:
                mid[lines, :] = more
            elif c < parts - 1:
                mid[lines, :] += more
            else:
                res[lines, :] = (mid[lines, :] + more).astype(BF16)
        give_back(low, high)
        for c in range(parts):
            exchange(w, c, lines).wait_send()

    def run(plan):
        for w, (low, high) in enumerate(plan):
            wave(w, low, high)

    if groups_of(n) == 2:
        pl.when(row == 0)(functools.partial(run, ((0, size), (size, n))))
        pl.when(row > 0)(functools.partial(run, ((0, n),)))
    else:
        run(((0, n),))

    keep(res, ret, r_recv)
    for copy in lend(rep):
        copy.wait_send()
    for group in range(len(send_groups)):
        if not (held and group == 1):
            sent(group)

    ids = ids_ref[...]
    gates = gates_ref[...]
    diagonal = iota((nodes, nodes), 0) == iota((nodes, nodes), 1)
    combined = None
    for group in range(len(recv_groups)):
        returned(group)
        lines = slice(group * size * cap, (group + 1) * size * cap)
        block = ret[lines, :]
        for k in range(ids.shape[0]):
            hit = jnp.where(ids[k : k + 1, :] == experts[lines], pick[lines], 0.0).astype(BF16)
            got = lax.dot_general(hit, block, over, preferred_element_type=F32)
            line = jnp.broadcast_to(gates[k : k + 1, :], (nodes, nodes))
            column = jnp.sum(jnp.where(diagonal, line, 0.0), axis=1, keepdims=True)
            combined = got * column if combined is None else combined + got * column
    out_ref[...] = combined
    drain(res, ret, n - 1 - held, r_send.at[0])


def grid_width(n):
    width = 1
    while width * width * 4 <= n:
        width *= 2
    return width


def body(tokens, expert_ids, gate_values, slot_expert, gate_weight, up_weight, down_weight):
    nodes, top = expert_ids.shape
    half = tokens.shape[1]
    n = slot_expert.shape[0]
    cap = nodes * top * 5 // (4 * (n // 2))
    hidden = gate_weight.shape[2]
    span = hidden
    parts = 2 * hidden // span
    groups = groups_of(n)
    hbm = pl.BlockSpec(memory_space=pl.ANY)
    dma = pltpu.SemaphoreType.DMA
    regular = pltpu.SemaphoreType.REGULAR

    combined = pl.pallas_call(
        functools.partial(kernel, n, cap),
        out_shape=pltpu.VMEM((nodes, half), F32),
        in_specs=[hbm] * 7,
        out_specs=pl.BlockSpec(memory_space=pltpu.VMEM),
        scratch_shapes=[
            pltpu.VMEM((nodes, half), BF16),
            pltpu.VMEM((top, nodes), jnp.int32),
            pltpu.VMEM((1, n), jnp.int32),
            pltpu.VMEM((top, nodes), F32),
            dma((4,)),
            pltpu.VMEM((2, half, hidden), BF16),
            pltpu.VMEM((2, half, hidden), BF16),
            pltpu.VMEM((2, hidden, half), BF16),
            dma((3,)), dma((3,)),
            dma((2 * groups - 1,)), dma((groups,)),
            dma, dma((groups, parts)),
            dma((groups,)), dma((groups,)),
            regular((max(n // grid_width(n) + grid_width(n) - 2, 1),)),
            regular, regular,
            pltpu.VMEM((n * cap, half), BF16),
            pltpu.VMEM((n * cap, half), BF16),
            pltpu.VMEM((n * cap, half), BF16),
            pltpu.VMEM((n * cap, half), BF16),
            pltpu.VMEM((parts, 2, n * cap, span), F32),
            pltpu.VMEM((parts, 2, n * cap, span), F32),
            pltpu.VMEM((n * cap, half), F32),
        ],
        compiler_params=pltpu.CompilerParams(
            collective_id=0, has_side_effects=True, vmem_limit_bytes=60000 * 1024
        ),
    )(tokens, expert_ids.T, slot_expert.reshape(1, n), gate_values.T,
      gate_weight, up_weight, down_weight)
    return combined.astype(BF16)


def solution(mesh):
    return jax.shard_map(
        body,
        mesh=mesh,
        in_specs=(
            P(("groups", "ep"), "rep"),
            P(("groups", "ep"), None),
            P(("groups", "ep"), None),
            P(),
            P("ep", None, "rep"),
            P("ep", None, "rep"),
            P("ep", "rep", None),
        ),
        out_specs=P(("groups", "ep"), "rep"),
        check_vma=False,
    )
```
